32 devices in a mesh: groups: 2 (over y), seq: 4 (over z), sample: 2 (over x), vocab: 2 (over core).
Axes of the slice: x: 2, y: 2, z: 4, core: 2. Of those that a mesh axis runs over, the one named last changes fastest.
Arguments:
- queries: bfloat16 [16, 256, 1792], P(('groups', 'sample'), 'seq', 'vocab'), parts along dimension 0, may hold values from -130 to 130
- key_states: bfloat16 [16, 256, 256], P(('groups', 'sample'), 'seq', 'vocab'), parts along dimension 0, may hold values from -8 to 8
- value_states: bfloat16 [16, 256, 256], P(('groups', 'sample'), 'seq', 'vocab'), parts along dimension 0, may hold values from -6 to 6
- residual: bfloat16 [16, 256, 1792], P(('groups', 'sample'), 'seq'), parts along dimension 0, may hold values from -3 to 3
- out_weight: bfloat16 [1792, 1792], P('vocab'), may hold values from -0.5 to 0.5
- norm_gain: float32 [1792], replicated, may hold values from 0.5 to 1.5
- vocab_head: bfloat16 [81920, 1792], P(('seq', 'sample', 'vocab')), may hold values from -21 to 21
- targets: int32 [16, 256], P(('groups', 'sample')), parts along dimension 0, may hold values from 0 to 81919
- scored_slots: int32 [16, 64], P(('groups', 'sample')), parts along dimension 0, may hold values from -1 to 255, as said below
- lengths: int32 [16], P(('groups', 'sample')), parts along dimension 0, may hold values from 64 to 256
- rewards: int32 [16], P(('groups', 'sample')), parts along dimension 0, may hold values from 0 to 4
Outputs:
- token_logprobs: float32 [16, 64], P(('groups', 'sample'), 'seq'), parts along dimension 0
- seq_scores: float32 [16], P(('groups', 'sample')), parts along dimension 0
- advantages: float32 [16], P(('groups', 'sample')), parts along dimension 0
- objective: float32 [2], P('groups'), parts along dimension 0
The draws below stay inside these ranges and needn't reach their ends.
There are 2 independent parts, one for each index of `groups`. The reference program is written for one: setup_inputs(seed, part) draws one part's arguments, and reference() takes and returns one part's arrays. A program takes and returns all parts, laid end to end along the dimension named above; an argument that names none is the same for every part. Nothing has to cross between parts.
Inputs may be any that keep to these rules, and one draw needn't show every extreme that they name: `scored_slots`: slots b * 16 to (b + 1) * 16 - 1 of a completion hold distinct positions of b * 64 to (b + 1) * 64 - 1 in rising order, followed by -1 in unused slots; every completion fills all 16 slots of some block; positions not listed are not scored. Positions from lengths[i] on are padding.
All inputs are finite; a program needn't handle non-finite values.
Results may differ from the reference program's by a relative error of at most 0.0085.
Values may be sent and summed in bfloat16 or wider, within the bound.
A program may use at most 128 MiB of HBM per device.

```python
import math
import jax
import jax.numpy as jnp
import numpy as np
from jax import lax

D = 1792
HQ = 14
HK = 2
HD = 128
V = 81920
K = 8
CH = 64
L = 256
CAP = 16


def attention_inputs(key):
    query_draw = jnp.clip(jax.random.normal(jax.random.fold_in(key, 11), (K, L, HQ * HD), jnp.float32), -6.0, 6.0)
    key_draw = jnp.clip(jax.random.normal(jax.random.fold_in(key, 12), (K, L, HK * HD), jnp.float32), -6.0, 6.0)
    return (query_draw, key_draw)


def draw_queries(key, part):
    return attention_inputs(key)[0].astype(jnp.bfloat16)


def draw_key_states(key, part):
    return attention_inputs(key)[1].astype(jnp.bfloat16)


def draw_vocab_head(key, part):
    base = jnp.clip(jax.random.normal(jax.random.fold_in(key, 21), (V, D), jnp.float32), -6.0, 6.0) * (3.0 / math.sqrt(D))
    return base.astype(jnp.bfloat16)


def draw_scored_slots(key, part):
    blocks = L // CH
    full_block = jax.random.randint(jax.random.fold_in(key, 31), (K,), 0, blocks)
    counts = jax.random.randint(jax.random.fold_in(key, 32), (K, blocks), CAP // 3, CAP + 1)
    counts = jnp.where(jnp.arange(blocks)[None, :] == full_block[:, None], CAP, counts)
    block_keys = jax.random.split(jax.random.fold_in(key, 33), K * blocks)
    picks = jax.vmap(lambda one_key: jnp.sort(jax.random.permutation(one_key, CH)[:CAP]))(block_keys)
    positions = picks.reshape(K, blocks, CAP) + (jnp.arange(blocks) * CH)[None, :, None]
    used = jnp.arange(CAP)[None, None, :] < counts[:, :, None]
    return jnp.where(used, positions, -1).reshape(K, blocks * CAP).astype(jnp.int32)


def with_ends(values, rng, least, largest):
    dims = values.shape
    spot = [jax.random.randint(jax.random.fold_in(rng, axis), (), 0, dims[axis]) for axis in range(len(dims))]
    values = values.at[tuple(spot)].set(least)
    longest = dims.index(max(dims))
    spot[longest] = (spot[longest] + 1) % dims[longest]
    return values.at[tuple(spot)].set(largest)


def shard_levels(own_key, extent, cuts, smallest, high):
    def one(axis_at, blocks):
        steps = jax.random.uniform(jax.random.fold_in(jax.random.fold_in(own_key, 6), axis_at), (blocks,), jnp.float32, smallest / len(cuts), high / len(cuts))
        return jnp.repeat(jnp.exp(steps), extent[axis_at] // blocks).reshape((-1,) + (1,) * (len(extent) - axis_at - 1))

    level = one(*cuts[0])
    for cut in cuts[1:]:
        level = level * one(*cut)
    return level


def skewed_wide(rng, extent, amount, slope):
    weights = [min(1 << octave, amount + 1 - (1 << octave)) * (1 << 20) // math.isqrt((1 << octave) ** slope) + 1 for octave in range((amount + 1).bit_length()) if 1 << octave <= amount]
    scale = 1 + sum(weights) // (1 << 30)
    table = np.cumsum(np.array([max(1, weight // scale) for weight in weights]))
    pick = jax.random.randint(jax.random.fold_in(rng, 1), extent, 0, int(table[len(weights) - 1]))
    start = jnp.left_shift(1, jnp.searchsorted(jnp.asarray(table, jnp.int32), pick, side="right").astype(jnp.int32))
    standing = start - 1 + jax.random.randint(jax.random.fold_in(rng, 4), extent, 0, 1 << 30) % jnp.minimum(start, amount + 1 - start)
    return jax.random.permutation(jax.random.fold_in(rng, 2), amount)[standing].astype(jnp.int32)


def scatter_about(own_key, shape, scale, reach, cuts=(), kind=jnp.bfloat16):
    gain = shard_levels(own_key, shape, cuts, -0.22, 0.18) if cuts else 1.0
    entries = jax.random.normal(own_key, shape, jnp.float32) * scale * gain
    return jnp.minimum(jnp.maximum(entries, -reach), reach).astype(kind)


def setup_inputs(seed: int = 0, part: int = 0) -> dict:
    key_list = jax.random.split(jax.random.key(seed), 12)
    own_keys = jax.random.split(jax.random.fold_in(key_list[11], part), 12)
    return {
        "queries": draw_queries(jax.random.fold_in(jax.random.fold_in(key_list[11], part), 71), part),
        "key_states": draw_key_states(jax.random.fold_in(jax.random.fold_in(key_list[11], part), 71), part),
        "value_states": scatter_about(own_keys[2], (K, L, HK * HD), 1.0, 6.0, ((0, 2), (1, 4), (2, 2))),
        "residual": scatter_about(own_keys[3], (K, L, D), 0.5, 3.0, ((0, 2), (1, 4))),
        "out_weight": scatter_about(key_list[4], (HQ * HD, D), (HQ * HD // 16) ** -0.5, 0.5, ((0, 2),)),
        "norm_gain": jnp.clip(1.0 + 0.1 * jax.random.normal(key_list[5], (D,), jnp.float32), 0.5, 1.5),
        "vocab_head": draw_vocab_head(jax.random.fold_in(key_list[11], 71), part),
        "targets": with_ends(skewed_wide(own_keys[7], (K, L), V, 2), jax.random.fold_in(own_keys[7], 3), 0, V - 1).astype(jnp.int32),
        "scored_slots": draw_scored_slots(jax.random.fold_in(jax.random.fold_in(key_list[11], part), 71), part),
        "lengths": with_ends(jax.random.randint(own_keys[9], (K,), L // 4, L + 1), jax.random.fold_in(own_keys[9], 1), L // 4, L).astype(jnp.int32),
        "rewards": with_ends(jax.random.randint(own_keys[10], (K,), 0, 5), jax.random.fold_in(own_keys[10], 1), 0, 4).astype(jnp.int32),
    }


def attend_sample(inputs):
    query_rows, key_rows, value_rows = inputs
    seq_len = query_rows.shape[0]
    group_size = HQ // HK
    query_view = query_rows.reshape(seq_len, HK, group_size, HD).astype(jnp.float32)
    key_view = key_rows.reshape(seq_len, HK, HD).astype(jnp.float32)
    value_view = value_rows.reshape(seq_len, HK, HD).astype(jnp.float32)
    scores = jnp.einsum('tkgd,skd->tkgs', query_view, key_view) * HD ** (-0.5)
    positions = jnp.arange(seq_len, dtype=jnp.int32)
    allowed = (positions[None, :] <= positions[:, None])[:, None, None, :]
    masked = jnp.where(allowed, scores, -1e+30)
    top_score = lax.optimization_barrier(jnp.max(masked, axis=-1, keepdims=True))
    exponent = jnp.where(allowed, jnp.exp(masked - top_score), 0.0)
    weight_sum = lax.optimization_barrier(jnp.sum(exponent, axis=-1))
    rounded = lax.optimization_barrier(exponent.astype(jnp.bfloat16))
    mixed = jnp.einsum('tkgs,skd->tkgd', rounded.astype(jnp.float32), value_view)
    return (mixed / weight_sum[..., None]).reshape(seq_len, HQ * HD).astype(jnp.bfloat16)

def score_rows(normed_rows, wanted, vocab_head):
    logits = jnp.dot(normed_rows, vocab_head.T, preferred_element_type=jnp.float32)
    top_score = lax.optimization_barrier(jnp.max(logits, axis=-1))
    weight_sum = lax.optimization_barrier(jnp.sum(jnp.exp(logits - top_score[:, None]), axis=-1))
    picked = jnp.take_along_axis(logits, wanted[:, None].astype(jnp.int32), axis=1)[:, 0]
    return picked - (top_score + jnp.log(weight_sum))

def reference(queries, key_states, value_states, residual, out_weight, norm_gain, vocab_head, targets, scored_slots, lengths, rewards):
    attended = lax.map(attend_sample, (queries, key_states, value_states))
    sample_count, seq_len, model_width = residual.shape
    partial_value = jnp.dot(attended.reshape(sample_count * seq_len, HQ * HD), out_weight, preferred_element_type=jnp.float32)
    hidden = residual.reshape(sample_count * seq_len, model_width).astype(jnp.float32) + partial_value
    power = lax.optimization_barrier(jnp.mean(hidden * hidden, axis=-1, keepdims=True))
    normed = (hidden * lax.rsqrt(power + 1e-06) * norm_gain).astype(jnp.bfloat16)
    normed = normed.reshape(sample_count, seq_len, model_width)
    slot_pos = jnp.maximum(scored_slots, 0).astype(jnp.int32)
    chosen = jnp.take_along_axis(normed, slot_pos[:, :, None], axis=1)
    wanted = jnp.take_along_axis(targets, slot_pos, axis=1)
    logprob = lax.map(lambda pair: score_rows(pair[0], pair[1], vocab_head), (chosen, wanted))
    scored = (scored_slots >= 0) & (scored_slots < lengths[:, None])
    token_logprobs = jnp.where(scored, logprob, 0.0)
    seq_scores = lax.optimization_barrier(jnp.sum(token_logprobs, axis=-1)) / seq_len
    reward_vals = rewards.astype(jnp.float32)
    reward_sum = jnp.sum(reward_vals)
    advantages = reward_vals - (reward_sum - reward_vals) / (K - 1)
    objective = -(jnp.sum(advantages * seq_scores) / K).reshape(1)
    return (token_logprobs, seq_scores, advantages, objective)
```

```python
import jax
import jax.numpy as jnp
from jax import lax
from jax.sharding import PartitionSpec as P

HD = 128
K = 8


floor_value = -1e30


def rms_scale(hidden, norm_gain):
    power = jnp.mean(hidden * hidden, axis=-1, keepdims=True)
    return (hidden * lax.rsqrt(power + 1e-06) * norm_gain).astype(jnp.bfloat16)


def shards(
    queries,
    key_states,
    value_states,
    residual,
    out_weight,
    norm_gain,
    vocab_head,
    targets,
    scored_slots,
    lengths,
    rewards,
):
    sample_count, block_len, query_width = queries.shape
    kv_heads = key_states.shape[2] // HD
    group_size = query_width // HD // kv_heads
    model_width = out_weight.shape[1]
    full_len = targets.shape[1]
    slot_total = scored_slots.shape[1]
    slot_cap = slot_total // lax.axis_size("seq")
    first_pos = lax.axis_index("seq") * block_len
    query_pos = first_pos + jnp.arange(block_len, dtype=jnp.int32)
    query_view = queries.reshape(sample_count, block_len, kv_heads, group_size, HD)
    stat_shape = (sample_count, block_len, kv_heads, group_size)
    pieces = (
        lax.all_gather(key_states, "seq", axis=1, tiled=True),
        lax.all_gather(value_states, "seq", axis=1, tiled=True),
    )
    top_score = jnp.full(stat_shape, floor_value, jnp.float32)
    piece_len = pieces[0].shape[1]
    key_view = pieces[0].reshape(sample_count, piece_len, kv_heads, HD)
    value_view = pieces[1].reshape(sample_count, piece_len, kv_heads, HD)
    scores = jnp.einsum(
        "srkgd,snkd->srkgn", query_view, key_view, preferred_element_type=jnp.float32
    ) * HD ** (-0.5)
    key_pos = jnp.arange(piece_len, dtype=jnp.int32)
    allowed = (key_pos[None, :] <= query_pos[:, None])[None, :, None, None, :]
    masked = jnp.where(allowed, scores, floor_value)
    new_top = jnp.maximum(top_score, jnp.max(masked, axis=-1))
    weights = jnp.where(allowed, jnp.exp(masked - new_top[..., None]), 0.0)
    weight_sum = jnp.sum(weights, axis=-1)
    update = jnp.einsum(
        "srkgn,snkd->srkgd",
        weights.astype(jnp.bfloat16),
        value_view,
        preferred_element_type=jnp.float32,
    )
    weighted = update
    new_top, weight_sum, weighted = (new_top, weight_sum, weighted)
    safe_sum = jnp.where(weight_sum > 0, weight_sum, 1.0)
    attended = (
        (weighted / safe_sum[..., None])
        .reshape(sample_count, block_len, query_width)
        .astype(jnp.bfloat16)
    )
    own_slots = lax.dynamic_slice_in_dim(
        scored_slots, lax.axis_index("seq") * slot_cap, slot_cap, 1
    )
    local_pos = jnp.clip(own_slots - first_pos, 0, block_len - 1)
    picked_attended = jnp.take_along_axis(attended, local_pos[:, :, None], axis=1)
    picked_resid = jnp.take_along_axis(residual, local_pos[:, :, None], axis=1)
    partial_value = jnp.einsum(
        "scq,qd->scd", picked_attended, out_weight, preferred_element_type=jnp.float32
    )
    shard_rows = vocab_head.shape[0]
    owner = (
        lax.axis_index("seq") * lax.axis_size("sample") + lax.axis_index("sample")
    ) * lax.axis_size("vocab") + lax.axis_index("vocab")
    vocab_ids = owner * shard_rows + jnp.arange(shard_rows, dtype=jnp.int32)
    summed = lax.psum(partial_value.astype(jnp.bfloat16), "vocab").astype(jnp.float32)
    normed = rms_scale(picked_resid.astype(jnp.float32) + summed, norm_gain)
    own_wanted = jnp.take_along_axis(targets, jnp.maximum(scored_slots, 0), axis=1)
    own_scored = (scored_slots >= 0) & (scored_slots < lengths[:, None])
    own_ints = jnp.concatenate(
        [own_wanted, own_scored.astype(jnp.int32), rewards[:, None]], axis=1
    )
    ints = lax.all_gather(own_ints, "sample", axis=0, tiled=True)
    wanted = ints[:, :slot_total]
    scored = ints[:, slot_total : 2 * slot_total] > 0
    reward_all = ints[:, 2 * slot_total].astype(jnp.float32)
    pieces = lax.all_gather(normed, ("sample", "seq"), axis=0)
    sample_size, seq_size = lax.axis_size("sample"), lax.axis_size("seq")
    pieces = pieces.reshape(sample_size, seq_size, sample_count, slot_cap, model_width)
    pieces = pieces.transpose(0, 2, 1, 3, 4)
    every_count = sample_size * sample_count
    flat = pieces.reshape(every_count * slot_total, model_width)
    logits = lax.dot_general(
        flat, vocab_head, (((1,), (1,)), ((), ())), preferred_element_type=jnp.float32
    )
    logits = logits.reshape(every_count, slot_total, shard_rows)
    top_local = jnp.max(logits, axis=-1)
    sum_local = jnp.sum(jnp.exp(logits - top_local[..., None]), axis=-1)
    picked = jnp.sum(jnp.where(vocab_ids[None, None, :] == wanted[..., None], logits, 0.0), axis=-1)
    stats = lax.all_gather(
        jnp.stack([top_local, sum_local, picked]), ("seq", "sample", "vocab"), axis=0
    )
    top_all = jnp.max(stats[:, 0], axis=0)
    sum_all = jnp.sum(stats[:, 1] * jnp.exp(stats[:, 0] - top_all), axis=0)
    pick_all = jnp.sum(stats[:, 2], axis=0)
    logprob = pick_all - (top_all + jnp.log(sum_all))
    token_all = jnp.where(scored, logprob, 0.0)
    score_all = jnp.sum(token_all, axis=-1) / full_len
    first = lax.axis_index("sample") * sample_count
    own_tokens = lax.dynamic_slice(
        token_all, (first, lax.axis_index("seq") * slot_cap), (sample_count, slot_cap)
    )
    own_scores = lax.dynamic_slice_in_dim(score_all, first, sample_count, 0)
    reward_sum = jnp.sum(reward_all)
    own_reward = rewards.astype(jnp.float32)
    own_advantage = own_reward - (reward_sum - own_reward) / (K - 1)
    every_advantage = reward_all - (reward_sum - reward_all) / (K - 1)
    objective = -(jnp.sum(every_advantage * score_all) / K).reshape(1)
    return (own_tokens, own_scores, own_advantage, objective)


def solution(mesh):
    in_specs = (
        P(("groups", "sample"), "seq", "vocab"),
        P(("groups", "sample"), "seq", "vocab"),
        P(("groups", "sample"), "seq", "vocab"),
        P(("groups", "sample"), "seq", None),
        P("vocab", None),
        P(),
        P(("seq", "sample", "vocab"), None),
        P(("groups", "sample"), None),
        P(("groups", "sample"), None),
        P(("groups", "sample")),
        P(("groups", "sample")),
    )
    out_specs = (
        P(("groups", "sample"), "seq"),
        P(("groups", "sample")),
        P(("groups", "sample")),
        P("groups"),
    )
    return jax.shard_map(shards, mesh=mesh, in_specs=in_specs, out_specs=out_specs, check_vma=False)
```

```python
import jax
import jax.numpy as jnp
from jax import lax
from jax.experimental import pallas as pl
from jax.experimental.pallas import tpu as pltpu
from jax.sharding import PartitionSpec as P

HD = 128
K = 8
MESH = pl.DeviceIdType.MESH
NT = (((1,), (1,)), ((), ()))


def block_rows(total):
    best = 16
    for rows in range(16, 513, 16):
        if total % rows == 0:
            best = rows
    return best


def kernel(
    q_ref, k_ref, v_ref, resid_ref, wo_ref, gain_ref, head_ref, pos_ref, meta_ref,
    token_ref, meta_out_ref,
    kv, resid_v, wo_v, head_v, att, part, xsend, xrecv, flat, meta, stats,
    load_sem, head_sem, kv_send, kv_recv, x_send, x_recv, f_send, f_recv,
    m_send, m_recv, s_send, s_recv,
):
    n_seq, n_samp, n_voc = flat.shape[1], flat.shape[0], flat.shape[2]
    count, block_len, query_width = q_ref.shape
    cap = pos_ref.shape[1]
    kv_heads = k_ref.shape[2] // HD
    group = query_width // HD // kv_heads
    nb = count // n_voc
    width = wo_ref.shape[1]
    slots = n_seq * count * cap
    s, m, w = lax.axis_index("seq"), lax.axis_index("sample"), lax.axis_index("vocab")
    me = (s * n_samp + m) * n_voc + w
    rows = block_rows(head_ref.shape[0])
    blocks = head_ref.shape[0] // rows

    def at(ds, dm, dw):
        return {
            "seq": lax.rem(s + ds, n_seq),
            "sample": lax.rem(m + dm, n_samp),
            "vocab": lax.rem(w + dw, n_voc),
        }

    peers = [
        (ds, dm, dw)
        for ds in range(n_seq)
        for dm in range(n_samp)
        for dw in range(n_voc)
        if (ds, dm, dw) != (0, 0, 0)
    ]

    loads = [
        pltpu.make_async_copy(k_ref, kv.at[s, 0], load_sem.at[0]),
        pltpu.make_async_copy(v_ref, kv.at[s, 1], load_sem.at[1]),
        pltpu.make_async_copy(wo_ref, wo_v, load_sem.at[2]),
        pltpu.make_async_copy(resid_ref, resid_v, load_sem.at[3]),
    ]
    for load in loads:
        load.start()

    barrier = pltpu.get_barrier_semaphore()
    for peer in peers:
        pl.semaphore_signal(barrier, inc=1, device_id=at(*peer), device_id_type=MESH)

    def head_copy(i):
        return pltpu.make_async_copy(
            head_ref.at[pl.ds(pl.multiple_of(i * rows, rows), rows)], head_v.at[i], head_sem.at[i]
        )

    for i in range(blocks):
        head_copy(i).start()

    for other in range(n_seq):

        @pl.when(other > s)
        def _():
            kv[other] = jnp.zeros(kv.shape[1:], kv.dtype)

    meta[m] = meta_ref[...]
    loads[0].wait()
    loads[1].wait()
    pl.semaphore_wait(barrier, len(peers))

    def kv_copy(origin, target, sem):
        return pltpu.make_async_remote_copy(
            src_ref=kv.at[origin],
            dst_ref=kv.at[origin],
            send_sem=kv_send.at[sem],
            recv_sem=kv_recv.at[origin],
            device_id={"seq": target},
            device_id_type=MESH,
        )

    for other in range(1, n_seq):

        @pl.when(other > s)
        def _():
            kv_copy(s, other, other).start()

    def meta_copy(owner, dm):
        return pltpu.make_async_remote_copy(
            src_ref=meta_ref,
            dst_ref=meta.at[owner],
            send_sem=m_send.at[dm],
            recv_sem=m_recv.at[owner],
            device_id={"sample": lax.rem(m + dm, n_samp)},
            device_id_type=MESH,
        )

    for dm in range(1, n_samp):
        meta_copy(m, dm).start()

    def onehot(b):
        lane = lax.broadcasted_iota(jnp.int32, (cap, block_len), 1)
        return jnp.where(lane == pos_ref[b], 1.0, 0.0).astype(jnp.bfloat16)

    picked = [
        jnp.dot(onehot(b), q_ref[b], preferred_element_type=jnp.float32).astype(jnp.bfloat16)
        for b in range(count)
    ]

    for other in range(n_seq - 1):

        @pl.when(other < s)
        def _():
            kv_copy(other, n_seq - 1, 0).wait_recv()

    for b in range(count):
        query_pos = pos_ref[b] + s * block_len
        query_pos = jnp.concatenate([query_pos] * group, axis=0)
        key_pos = lax.broadcasted_iota(jnp.int32, (group * cap, n_seq * block_len), 1)
        allowed = key_pos <= query_pos
        for g in range(kv_heads):
            keys = kv[:, 0, b, :, g * HD : (g + 1) * HD].reshape(n_seq * block_len, HD)
            values = kv[:, 1, b, :, g * HD : (g + 1) * HD].reshape(n_seq * block_len, HD)
            cols = [(g * group + h) * HD for h in range(group)]
            query = jnp.concatenate([picked[b][:, c : c + HD] for c in cols], axis=0)
            scores = lax.dot_general(query, keys, NT, preferred_element_type=jnp.float32)
            masked = jnp.where(allowed, scores * HD ** (-0.5), -1e30)
            top = jnp.max(masked, axis=1, keepdims=True)
            weights = jnp.where(allowed, jnp.exp(masked - top), 0.0)
            total = jnp.sum(weights, axis=1, keepdims=True)
            mixed = jnp.dot(
                weights.astype(jnp.bfloat16), values, preferred_element_type=jnp.float32
            )
            mixed = (mixed / total).astype(jnp.bfloat16)
            for h in range(group):
                att[b * cap : (b + 1) * cap, cols[h] : cols[h] + HD] = mixed[
                    h * cap : (h + 1) * cap
                ]

    loads[2].wait()
    product = jnp.dot(att[...], wo_v[...], preferred_element_type=jnp.float32)
    part[...] = product.reshape(part.shape)
    xsend[...] = product.astype(jnp.bfloat16).reshape(xsend.shape)

    def x_copy(owner, dw):
        target = lax.rem(w + dw, n_voc)
        return pltpu.make_async_remote_copy(
            src_ref=xsend.at[target],
            dst_ref=xrecv.at[owner],
            send_sem=x_send.at[dw],
            recv_sem=x_recv.at[owner],
            device_id={"vocab": target},
            device_id_type=MESH,
        )

    for dw in range(1, n_voc):
        x_copy(w, dw).start()
    loads[3].wait()
    hidden = [
        part[w, i]
        + jnp.dot(
            onehot(w * nb + i), resid_v[w * nb + i], preferred_element_type=jnp.float32
        )
        for i in range(nb)
    ]
    for dw in range(1, n_voc):
        owner = lax.rem(w + dw, n_voc)
        x_copy(owner, dw).wait_recv()
        hidden = [hidden[i] + xrecv[owner, i].astype(jnp.float32) for i in range(nb)]
    for i in range(nb):
        power = jnp.mean(hidden[i] * hidden[i], axis=-1, keepdims=True)
        normed = hidden[i] * lax.rsqrt(power + 1e-06) * gain_ref[...]
        flat[m, s, w, i] = normed.astype(jnp.bfloat16)

    def piece_copy(piece, sem, device):
        return pltpu.make_async_remote_copy(
            src_ref=flat.at[piece],
            dst_ref=flat.at[piece],
            send_sem=f_send.at[sem],
            recv_sem=f_recv.at[piece],
            device_id=device,
            device_id_type=MESH,
        )

    n_kind = n_samp + n_voc - 2

    def forward(dm0, ds):
        piece = (lax.rem(m + dm0, n_samp), lax.rem(s + ds, n_seq), w)
        base = (n_seq - 1) + (dm0 * n_seq + ds) * n_kind
        out = []
        if dm0 == 0:
            for dm in range(1, n_samp):
                out.append(piece_copy(piece, base + dm - 1, {"sample": lax.rem(m + dm, n_samp)}))
        for dw in range(1, n_voc):
            out.append(
                piece_copy(
                    piece, base + n_samp - 2 + dw, {"vocab": lax.rem(w + dw, n_voc)}
                )
            )
        return out

    def arrival(dm0, ds, dw):
        piece = (lax.rem(m + dm0, n_samp), lax.rem(s + ds, n_seq), lax.rem(w + dw, n_voc))
        return piece_copy(piece, 0, {"vocab": lax.rem(w + 1, n_voc)})

    def along(ds):
        return piece_copy((m, s, w), ds - 1, {"seq": lax.rem(s + ds, n_seq)})

    for ds in range(1, n_seq):
        along(ds).start()
    for copy in forward(0, 0):
        copy.start()
    order = sorted(range(1, n_seq), key=lambda ds: min(ds, n_seq - ds))
    for ds in order:
        arrival(0, ds, 0).wait_recv()
        for copy in forward(0, ds):
            copy.start()
    for ds in range(n_seq):
        for dw in range(1, n_voc):
            arrival(0, ds, dw).wait_recv()
    for dm in range(1, n_samp):
        meta_copy(lax.rem(m + dm, n_samp), dm).wait_recv()

    late = blocks - n_seq

    def relay(dm0, ds):
        arrival(dm0, ds, 0).wait_recv()
        for copy in forward(dm0, ds):
            copy.start()

    for dm0 in range(n_samp):
        piece_m = lax.rem(m + dm0, n_samp)
        if dm0 > 0:
            for ds in range(n_seq):
                for dw in range(1, n_voc):
                    arrival(dm0, ds, dw).wait_recv()
        wanted = meta[piece_m][:, :slots]

        def step(i, carry, dm0=dm0, piece_m=piece_m, wanted=wanted):
            top, total, pick = carry
            if dm0 == 0:
                head_copy(i).wait()
            if dm0 + 1 < n_samp and late >= 0:

                @pl.when(i >= late)
                def _():
                    relay(dm0 + 1, i - late)

            logits = lax.dot_general(
                head_v[i],
                flat[piece_m].reshape(slots, width),
                NT,
                preferred_element_type=jnp.float32,
            )
            new_top = jnp.maximum(top, jnp.max(logits, axis=0, keepdims=True))
            total = total * jnp.exp(top - new_top) + jnp.sum(
                jnp.exp(logits - new_top), axis=0, keepdims=True
            )
            ids = lax.broadcasted_iota(jnp.int32, (rows, slots), 0)
            hit = ids == wanted - (me * blocks + i) * rows
            pick = pick + jnp.sum(jnp.where(hit, logits, 0.0), axis=0, keepdims=True)
            return new_top, total, pick

        init = (
            jnp.full((1, slots), -1e30, jnp.float32),
            jnp.zeros((1, slots), jnp.float32),
            jnp.zeros((1, slots), jnp.float32),
        )
        done = lax.fori_loop(0, blocks, step, init)
        if dm0 + 1 < n_samp and late < 0:
            for ds in range(n_seq):
                relay(dm0 + 1, ds)
        for part_at in range(3):
            stats[me, part_at, piece_m] = done[part_at]

    def stat_copy(owner, sem, device):
        return pltpu.make_async_remote_copy(
            src_ref=stats.at[owner],
            dst_ref=stats.at[owner],
            send_sem=s_send.at[sem],
            recv_sem=s_recv.at[owner],
            device_id=device,
            device_id_type=MESH,
        )

    for sem, peer in enumerate(peers):
        stat_copy(me, sem, at(*peer)).start()
    for sem, peer in enumerate(peers):
        where = at(*peer)
        owner = (where["seq"] * n_samp + where["sample"]) * n_voc + where["vocab"]
        stat_copy(owner, sem, where).wait_recv()
    for sample in range(n_samp):
        tops = stats[:, 0, sample]
        top_all = jnp.max(tops, axis=0)
        sum_all = jnp.sum(stats[:, 1, sample] * jnp.exp(tops - top_all), axis=0)
        logprob = jnp.sum(stats[:, 2, sample], axis=0) - (top_all + jnp.log(sum_all))
        info = meta[sample]
        token_ref[sample] = jnp.where(info[:, slots : 2 * slots] > 0, logprob, 0.0)
        meta_out_ref[sample] = info[:, 2 * slots :]

    for other in range(1, n_seq):

        @pl.when(other > s)
        def _():
            kv_copy(s, other, other).wait_send()

    for dm in range(1, n_samp):
        meta_copy(m, dm).wait_send()
    for dw in range(1, n_voc):
        x_copy(w, dw).wait_send()
    for ds in range(1, n_seq):
        along(ds).wait_send()
    for dm0 in range(n_samp):
        for ds in range(n_seq):
            for copy in forward(dm0, ds):
                copy.wait_send()
    for sem, peer in enumerate(peers):
        stat_copy(me, sem, at(*peer)).wait_send()


def shards(
    queries,
    key_states,
    value_states,
    residual,
    out_weight,
    norm_gain,
    vocab_head,
    targets,
    scored_slots,
    lengths,
    rewards,
):
    count, block_len, query_width = queries.shape
    width = out_weight.shape[1]
    full_len = targets.shape[1]
    slot_total = scored_slots.shape[1]
    n_seq, n_samp, n_voc = (lax.axis_size(a) for a in ("seq", "sample", "vocab"))
    cap = slot_total // n_seq
    slots = slot_total * count
    s, m = lax.axis_index("seq"), lax.axis_index("sample")
    nb = count // n_voc
    rows = block_rows(vocab_head.shape[0])
    blocks = vocab_head.shape[0] // rows
    own_slots = lax.dynamic_slice_in_dim(scored_slots, s * cap, cap, 1)
    local_pos = jnp.clip(own_slots - s * block_len, 0, block_len - 1)[..., None]
    wanted = jnp.take_along_axis(targets, jnp.maximum(scored_slots, 0), axis=1)
    scored = (scored_slots >= 0) & (scored_slots < lengths[:, None])

    def by_block(values):
        return values.reshape(count, n_seq, cap).transpose(1, 0, 2).reshape(1, slots)

    pad = 128 - count
    meta_in = jnp.concatenate(
        [by_block(wanted), by_block(scored.astype(jnp.int32)), jnp.pad(rewards, (0, pad))[None]],
        axis=1,
    )
    n_dev = n_seq * n_samp * n_voc
    vmem = pl.BlockSpec(memory_space=pltpu.VMEM)
    hbm = pl.BlockSpec(memory_space=pl.ANY)
    bf16, f32 = jnp.bfloat16, jnp.float32
    dma = pltpu.SemaphoreType.DMA
    n_send = n_seq - 1 + n_seq * n_samp * (n_samp + n_voc - 2)
    token, reward = pl.pallas_call(
        kernel,
        out_shape=(
            jax.ShapeDtypeStruct((n_samp, 1, slots), f32),
            jax.ShapeDtypeStruct((n_samp, 1, 128), jnp.int32),
        ),
        in_specs=[vmem, hbm, hbm, hbm, hbm, vmem, hbm, vmem, vmem],
        out_specs=(vmem, vmem),
        scratch_shapes=[
            pltpu.VMEM((n_seq, 2) + key_states.shape, bf16),
            pltpu.VMEM(residual.shape, bf16),
            pltpu.VMEM(out_weight.shape, bf16),
            pltpu.VMEM((blocks, rows, width), bf16),
            pltpu.VMEM((count * cap, query_width), bf16),
            pltpu.VMEM((n_voc, nb, cap, width), f32),
            pltpu.VMEM((n_voc, nb, cap, width), bf16),
            pltpu.VMEM((n_voc, nb, cap, width), bf16),
            pltpu.VMEM((n_samp, n_seq, n_voc, nb, cap, width), bf16),
            pltpu.VMEM((n_samp, 1, 2 * slots + 128), jnp.int32),
            pltpu.VMEM((n_dev, 3, n_samp, 1, slots), f32),
            dma((4,)),
            dma((blocks,)),
            dma((n_seq,)),
            dma((n_seq,)),
            dma((n_voc,)),
            dma((n_voc,)),
            dma((n_send,)),
            dma((n_samp, n_seq, n_voc)),
            dma((n_samp,)),
            dma((n_samp,)),
            dma((n_dev - 1,)),
            dma((n_dev,)),
        ],
        compiler_params=pltpu.CompilerParams(
            collective_id=0, has_side_effects=True, vmem_limit_bytes=60 * 1024 * 1024
        ),
    )(
        queries, key_states, value_states, residual, out_weight, norm_gain[None],
        vocab_head, local_pos, meta_in,
    )
    token = token.reshape(n_samp, n_seq, count, cap)
    reward_all = reward[:, 0, :count].astype(f32).reshape(-1)
    score_all = (jnp.sum(token, axis=(1, 3)) / full_len).reshape(-1)
    own_tokens = lax.dynamic_slice(token, (m, s, 0, 0), (1, 1, count, cap))[0, 0]
    own_scores = lax.dynamic_slice_in_dim(score_all, m * count, count, 0)
    reward_sum = jnp.sum(reward_all)
    own_reward = rewards.astype(f32)
    own_advantage = own_reward - (reward_sum - own_reward) / (K - 1)
    every_advantage = reward_all - (reward_sum - reward_all) / (K - 1)
    objective = -(jnp.sum(every_advantage * score_all) / K).reshape(1)
    return (own_tokens, own_scores, own_advantage, objective)


def solution(mesh):
    in_specs = (
        P(("groups", "sample"), "seq", "vocab"),
        P(("groups", "sample"), "seq", "vocab"),
        P(("groups", "sample"), "seq", "vocab"),
        P(("groups", "sample"), "seq", None),
        P("vocab", None),
        P(),
        P(("seq", "sample", "vocab"), None),
        P(("groups", "sample"), None),
        P(("groups", "sample"), None),
        P(("groups", "sample")),
        P(("groups", "sample")),
    )
    out_specs = (
        P(("groups", "sample"), "seq"),
        P(("groups", "sample")),
        P(("groups", "sample")),
        P("groups"),
    )
    return jax.shard_map(shards, mesh=mesh, in_specs=in_specs, out_specs=out_specs, check_vma=False)
```
